32 devices in a mesh: image: 2 (over y), ga: 4 (over z), band: 4 (over x, core).
Axes of the slice: x: 2, y: 2, z: 4, core: 2. Of those that a mesh axis runs over, the one named last changes fastest.
Arguments:
- projectors: bfloat16 [160, 655360], P(('image', 'band'), 'ga'), parts along dimension 0, may hold values from -6 to 6
- occupied: bfloat16 [256, 655360], P(('image', 'band'), 'ga'), parts along dimension 0, may hold values from -0.0009765625 to 0.0009765625
- block: bfloat16 [512, 655360], P(('image', 'band'), 'ga'), parts along dimension 0, may hold values from -0.0078125 to 0.0078125
- weights: float32 [256], P(('image', 'band')), parts along dimension 0, may hold values from 0.1 to 1
- u_index: int32 [16], replicated, may hold values from 0 to 3
- u_values: float32 [4], replicated, may hold values from 0.5 to 2
Outputs:
- applied: bfloat16 [512, 655360], P(('image', 'band'), 'ga'), parts along dimension 0
The draws below stay inside these ranges and needn't reach their ends.
There are 2 independent parts, one for each index of `image`. The reference program is written for one: setup_inputs(seed, part) draws one part's arguments, and reference() takes and returns one part's arrays. A program takes and returns all parts, laid end to end along the dimension named above; an argument that names none is the same for every part. Nothing has to cross between parts.
Inputs may be any that keep to these rules, and one draw needn't show every extreme that they name: `u_index`: each atom's entry of the U table.
All inputs are finite; a program needn't handle non-finite values.
Results may differ from the reference program's by a relative error of at most 0.0049.
Values may be sent and summed in bfloat16 or wider, within the bound.
No kernel may reach another device: no remote copies, remote signals or barrier semaphores. Data moves between devices by JAX's collectives and lax.ppermute only.
A program may use at most 192 MiB of HBM per device.

```python
import math
import jax
import jax.numpy as jnp
from jax import lax

NPW = 655360
ORB = 5
NAT = 16
NSPEC = 4
NOCC = 128
NBLK = 256
NPROJ = 80


def place_ends(drawn, key, low, top_value):
    longest = drawn.shape.index(max(drawn.shape))
    spots = []
    for shift in (0, 1):
        where = [jax.random.randint(jax.random.fold_in(key, axis), (), 0, length) for axis, length in enumerate(drawn.shape)]
        where[longest] = (where[longest] + shift) % drawn.shape[longest]
        spots.append(tuple(where))
    return drawn.at[spots[0]].set(low).at[spots[1]].set(top_value)


def levels(own_key, dims, shards, least, top_value):
    def one(position, parts):
        steps = jax.random.uniform(jax.random.fold_in(jax.random.fold_in(own_key, 6), position), (parts,), jnp.float32, least / len(shards), top_value / len(shards))
        return jnp.repeat(jnp.exp(steps), dims[position] // parts).reshape((-1,) + (1,) * (len(dims) - position - 1))

    gain = one(*shards[0])
    for cut in shards[1:]:
        gain = gain * one(*cut)
    return gain


def bell_draw(rng, dims, spread, most, pieces=(), kind=jnp.bfloat16):
    values = spread * jax.random.normal(rng, dims, jnp.float32)
    if pieces:
        values = values * levels(rng, dims, pieces, -0.22, 0.18)
    return jnp.clip(values, -most, most).astype(kind)


def setup_inputs(seed: int = 0, part: int = 0) -> dict:
    key_of = jax.random.split(jax.random.key(seed), 7)
    part_keys = jax.random.split(jax.random.fold_in(key_of[6], part), 7)
    return {
        "projectors": bell_draw(part_keys[0], (NPROJ, NPW), 1.0, 6.0, ((0, 4), (1, 4))),
        "occupied": bell_draw(part_keys[1], (NOCC, NPW), (NPW * NOCC // 2) ** -0.5, 0.0009765625, ((0, 4), (1, 4))),
        "block": bell_draw(part_keys[2], (NBLK, NPW), NPW ** -0.5, 0.0078125, ((0, 4), (1, 4))),
        "weights": jnp.clip(jnp.exp(math.log(1.0) - 2.3025851 * jax.random.uniform(part_keys[3], (NOCC,), jnp.float32) ** levels(part_keys[3], (NOCC,), ((0, 4),), -0.2, 0.2)), 0.1, 1.0),
        "u_index": place_ends(jax.random.randint(key_of[4], (NAT,), 0, NSPEC), jax.random.fold_in(key_of[4], 1), 0, NSPEC - 1).astype(jnp.int32),
        "u_values": jnp.clip(jnp.exp(jax.random.uniform(key_of[5], (NSPEC,), jnp.float32, math.log(0.5), math.log(2.0))), 0.5, 2.0),
    }


def reference(projectors, occupied, block, weights, u_index, u_values):
    proj_occ = jnp.dot(projectors, occupied.T, preferred_element_type=jnp.float32)
    proj_blk = jnp.dot(projectors, block.T, preferred_element_type=jnp.float32)
    shaped = proj_occ.reshape(NAT, ORB, NOCC)
    occ = jnp.einsum("amb,anb->amn", shaped * weights[None, None, :], shaped, precision=lax.Precision.HIGHEST)
    selector = (u_index[:, None] == jnp.arange(NSPEC, dtype=jnp.int32)[None, :]).astype(jnp.float32)
    u_atom = jnp.dot(selector, u_values, precision=lax.Precision.HIGHEST)
    potential = u_atom[:, None, None] * (0.5 * jnp.eye(ORB, dtype=jnp.float32)[None] - occ)
    hub_coef = jnp.einsum("amn,anc->amc", potential, proj_blk.reshape(NAT, ORB, NBLK), precision=lax.Precision.HIGHEST)
    hub_coef = hub_coef.reshape(NPROJ, NBLK).astype(jnp.bfloat16)
    applied = jnp.dot(hub_coef.T, projectors, preferred_element_type=jnp.float32)
    return applied.astype(jnp.bfloat16)
```

```python
import functools

import jax
import jax.numpy as jnp
import numpy as np
from jax import lax
from jax.experimental import pallas as pl
from jax.experimental.pallas import tpu as pltpu
from jax.sharding import PartitionSpec as P

ORB = 5
SUBLANES = 8
LANES = 128
PLAN = (1, 5, 6, 6, 6, 6, 6, 3, 1)
HIGH = lax.Precision.HIGHEST
NT = (((1,), (1,)), ((), ()))
NN = (((1,), (0,)), ((), ()))
TN = (((0,), (0,)), ((), ()))


def exact_dot(left, right, dims):
    return lax.dot_general(
        left, right, dims, precision=HIGH, preferred_element_type=jnp.float32
    )


def contract_kernel(quarters, groups, *refs):
    row_refs = refs[:quarters]
    band_refs = refs[quarters : quarters + 2 * groups]
    acc_in, packed_ref, acc_ref = refs[quarters + 2 * groups :]
    rows = row_refs[0].shape[0]

    @pl.when(pl.program_id(0) == 0)
    def _():
        acc_ref[...] = acc_in[...]

    for place, ref in enumerate(row_refs):
        packed_ref[place * rows : (place + 1) * rows, :] = ref[...]
    bands = jnp.concatenate([ref[...] for ref in band_refs], axis=0)
    acc_ref[...] += lax.dot_general(
        bands, packed_ref[...], NT, preferred_element_type=jnp.float32
    )


def contract_chunk(parts, occupied, block, acc, first, groups, tile):
    rows, width = parts[0].shape
    steps = width // tile
    group_steps = occupied.shape[1] // groups // tile
    start = first // tile
    specs = [pl.BlockSpec((rows, tile), lambda i: (0, i)) for _ in parts]
    operands = list(parts)
    for bands in (occupied, block):
        for group in range(groups):
            offset = start + group * group_steps
            specs.append(
                pl.BlockSpec((bands.shape[0], tile), lambda i, offset=offset: (0, i + offset))
            )
            operands.append(bands)
    specs.append(pl.BlockSpec(acc.shape, lambda i: (0, 0)))
    operands.append(acc)
    depth = rows * len(parts)
    return pl.pallas_call(
        functools.partial(contract_kernel, len(parts), groups),
        grid=(steps,),
        in_specs=specs,
        out_specs=[
            pl.BlockSpec((depth, tile), lambda i: (0, i)),
            pl.BlockSpec(acc.shape, lambda i: (0, 0)),
        ],
        out_shape=[
            jax.ShapeDtypeStruct((depth, width), parts[0].dtype),
            jax.ShapeDtypeStruct(acc.shape, acc.dtype),
        ],
        compiler_params=pltpu.CompilerParams(vmem_limit_bytes=16 * 2**20),
        cost_estimate=pl.CostEstimate(
            flops=2 * acc.shape[0] * depth * width * 4,
            bytes_accessed=2 * width * (2 * depth + acc.shape[0]),
            transcendentals=0,
        ),
        name="contract",
    )(*operands)


def fold_kernel(groups, occ_bands, blk_bands, acc_ref, mask_ref, fold_ref, out_ref):
    acc = acc_ref[...]
    mask = mask_ref[...]
    occ = jnp.zeros((occ_bands, acc.shape[1]), jnp.float32)
    blk = jnp.zeros((blk_bands, acc.shape[1]), jnp.float32)
    base = groups * occ_bands
    for group in range(groups):
        keep = mask[group : group + 1, :]
        occ += acc[group * occ_bands : (group + 1) * occ_bands, :] * keep
        blk += acc[base + group * blk_bands : base + (group + 1) * blk_bands, :] * keep
    out_ref[...] = exact_dot(jnp.concatenate([occ, blk], axis=0), fold_ref[...], NN)


def occupation_kernel(count, occ_bands, *refs):
    parts = refs[:count]
    weights_ref, same_atom_ref, narrow_ref, blk_ref, occ_ref = refs[count:]
    total = parts[0][...]
    for ref in parts[1:]:
        total = total + ref[...]
    occ_rows = total[:occ_bands, :]
    gram = exact_dot(occ_rows * weights_ref[...], occ_rows, TN) * same_atom_ref[...]
    occ_ref[...] = exact_dot(gram, narrow_ref[...], NN)
    blk_ref[...] = total[occ_bands:, :]


def apply_kernel(widths, count, groups, tile, *refs):
    chunk_refs = refs[: len(widths)]
    occ_refs = refs[len(widths) : len(widths) + count]
    rest = refs[len(widths) + count :]
    orders_ref, blk_ref, u_ref, half_ref, same_atom_ref, narrow_ref, fold_ref, mask_ref = rest[:8]
    out_ref, coef_ref, stage_ref, sems = rest[8:]
    step = pl.program_id(0)
    bands = blk_ref.shape[0]
    group_width = out_ref.shape[1] // groups
    slots = stage_ref.shape[0]
    steps = pl.num_programs(0)

    @pl.when(step == 0)
    def _():
        occ = occ_refs[0][...]
        for shift in range(1, count):
            occ += exact_dot(orders_ref[shift], occ_refs[shift][...], NN)
        wide = exact_dot(occ, narrow_ref[...], NT) * same_atom_ref[...]
        potential = u_ref[...] * (half_ref[...] - wide)
        hub = exact_dot(blk_ref[...], potential, NT).astype(jnp.bfloat16)
        spread = lax.dot_general(
            hub, fold_ref[...].astype(jnp.bfloat16), NT, preferred_element_type=jnp.float32
        )
        for group in range(groups):
            coef_ref[group * bands : (group + 1) * bands, :] = (
                spread * mask_ref[group : group + 1, :]
            ).astype(jnp.bfloat16)

    def copies(at):
        slot = lax.rem(at, slots)
        return [
            pltpu.make_async_copy(
                stage_ref.at[slot, pl.ds(group * bands, bands), :],
                out_ref.at[:, pl.ds(pl.multiple_of(group * group_width + at * tile, tile), tile)],
                sems.at[slot, group],
            )
            for group in range(groups)
        ]

    @pl.when(step >= slots)
    def _():
        for copy in copies(step - slots):
            copy.wait()

    begin = 0
    for ref, width in zip(chunk_refs, widths):
        end = begin + width // tile

        @pl.when((step >= begin) & (step < end))
        def _(ref=ref):
            stage_ref[lax.rem(step, slots)] = jnp.dot(
                coef_ref[...], ref[...], preferred_element_type=jnp.float32
            ).astype(jnp.bfloat16)

        begin = end

    for copy in copies(step):
        copy.start()

    @pl.when(step == steps - 1)
    def _():
        for back in range(min(slots, sum(widths) // tile) - 1, -1, -1):
            for copy in copies(step - back):
                copy.wait()


def apply_all(chunks, occs, orders, blk, u_rows, half, same_atom, narrow, fold, mask, columns, groups, tile):
    widths = [chunk.shape[1] for chunk in chunks]
    depth = chunks[0].shape[0]
    bands = blk.shape[0]
    specs, begin = [], 0
    for width in widths:
        count = width // tile
        specs.append(
            pl.BlockSpec(
                (depth, tile),
                lambda i, begin=begin, count=count: (0, jnp.clip(i - begin, 0, count - 1)),
            )
        )
        begin += count
    small = [*occs, orders, blk, u_rows, half, same_atom, narrow, fold, mask]
    for value in small:
        specs.append(pl.BlockSpec(value.shape, lambda i, rank=value.ndim: (0,) * rank))
    slots = 3
    return pl.pallas_call(
        functools.partial(apply_kernel, widths, len(occs), groups, tile),
        grid=(begin,),
        in_specs=specs,
        out_specs=pl.BlockSpec(memory_space=pl.ANY),
        out_shape=jax.ShapeDtypeStruct((bands, columns), jnp.bfloat16),
        scratch_shapes=[
            pltpu.VMEM((groups * bands, depth), jnp.bfloat16),
            pltpu.VMEM((slots, groups * bands, tile), jnp.bfloat16),
            pltpu.SemaphoreType.DMA((slots, groups)),
        ],
        compiler_params=pltpu.CompilerParams(vmem_limit_bytes=24 * 2**20),
        cost_estimate=pl.CostEstimate(
            flops=2 * groups * bands * depth * sum(widths),
            bytes_accessed=2 * (depth * sum(widths) + bands * columns),
            transcendentals=0,
        ),
        name="apply",
    )(*chunks, *small)


def swap(value, bit, size):
    return lax.ppermute(value, "band", [(i, i ^ bit) for i in range(size)])


def turn(value, shift, size):
    return lax.ppermute(value, "ga", [(i, (i + shift) % size) for i in range(size)])


def per_device(band_size, ga_size, projectors, occupied, block, weights, u_index, u_values):
    rows, columns = projectors.shape
    occ_bands, blk_bands = occupied.shape[0], block.shape[0]
    total = rows * band_size
    groups = 1
    while rows * groups % SUBLANES:
        groups *= 2
    length = columns // groups
    units = sum(PLAN)
    tile = length // units
    if length % units or tile % LANES or rows % ORB or band_size & (band_size - 1):
        raise ValueError("unsupported shape")

    plain = np.arange(total)
    packed = np.arange(total * groups)
    packed_quarter, packed_group = packed // (rows * groups), packed // rows % groups
    fold = (packed_quarter * rows + packed % rows)[:, None] == plain[None, :]
    mask = packed_group[None, :] == np.arange(groups)[:, None]
    same_atom = (plain // ORB)[:, None] == (plain // ORB)[None, :]
    narrow = (plain % rows)[:, None] == np.arange(rows)[None, :]
    moved = [((plain // rows) ^ shift) * rows + plain % rows for shift in range(band_size)]
    orders = np.stack([order[:, None] == plain[None, :] for order in moved])
    fold, mask, same_atom, narrow, orders, half = (
        jnp.asarray(np.asarray(value, np.float32))
        for value in (fold, mask, same_atom, narrow, orders, 0.5 * np.eye(total))
    )

    here = lax.axis_index("band")
    atom = ((plain // rows) ^ here) * (rows // ORB) + plain % rows // ORB
    selector = (u_index[:, None] == jnp.arange(u_values.shape[0], dtype=jnp.int32)[None, :]).astype(
        jnp.float32
    )
    u_atom = jnp.dot(selector, u_values, precision=HIGH)
    picks = (atom[:, None] == jnp.arange(u_index.shape[0])[None, :]).astype(jnp.float32)
    u_rows = jnp.dot(picks, u_atom[:, None], precision=HIGH)

    bits = []
    bit = band_size // 2
    while bit:
        bits.append(bit)
        bit //= 2

    acc = jnp.zeros((groups * (occ_bands + blk_bands), total * groups), jnp.float32)
    chunks, first = [], 0
    for share in PLAN:
        width = share * tile
        piece = jnp.concatenate(
            [
                projectors[:, group * length + first : group * length + first + width]
                for group in range(groups)
            ],
            axis=0,
        )
        held = {0: piece}
        for bit in bits:
            held.update({place ^ bit: swap(value, bit, band_size) for place, value in held.items()})
        parts = [held[place] for place in range(band_size)]
        chunk, acc = contract_chunk(parts, occupied, block, acc, first, groups, tile)
        chunks.append(chunk)
        first += width

    partial = pl.pallas_call(
        functools.partial(fold_kernel, groups, occ_bands, blk_bands),
        out_shape=jax.ShapeDtypeStruct((occ_bands + blk_bands, total), jnp.float32),
        name="fold",
    )(acc, mask, fold)
    partials = [partial] + [turn(partial, shift, ga_size) for shift in range(1, ga_size)]
    proj_blk, occ = pl.pallas_call(
        functools.partial(occupation_kernel, ga_size, occ_bands),
        out_shape=[
            jax.ShapeDtypeStruct((blk_bands, total), jnp.float32),
            jax.ShapeDtypeStruct((total, rows), jnp.float32),
        ],
        name="occupations",
    )(*partials, weights[:, None], same_atom, narrow)
    occs = [occ] + [swap(occ, shift, band_size) for shift in range(1, band_size)]
    return apply_all(
        chunks, occs, orders, proj_blk, u_rows, half, same_atom, narrow, fold, mask,
        columns, groups, tile,
    )


def solution(mesh):
    in_specs = (
        P(("image", "band"), "ga"),
        P(("image", "band"), "ga"),
        P(("image", "band"), "ga"),
        P(("image", "band")),
        P(),
        P(),
    )
    out_specs = P(("image", "band"), "ga")
    return jax.shard_map(
        functools.partial(per_device, mesh.shape["band"], mesh.shape["ga"]),
        mesh=mesh,
        in_specs=in_specs,
        out_specs=out_specs,
        check_vma=False,
    )
```
